256 devices in a mesh: px: 4 (over y), py: 8 (over z), fr: 8 (over x, core).
Axes of the slice: x: 4, y: 4, z: 8, core: 2. Of those that a mesh axis runs over, the one named last changes fastest.
Arguments:
- frames: bfloat16 [32, 2048, 2048], P('fr', 'px', 'py'), may hold values from 0.019897461 to 1
- a_start: float32 [64, 2048], P(None, 'px'), may hold values from 0.1 to 1
- b_start: float32 [64, 2048], P(None, 'py'), may hold values from 0.1 to 10, as said below
- c_start: float32 [64, 32], P(None, 'fr'), may hold values from 0.1 to 10, as said below
Outputs:
- a_factor: float32 [64, 2048], P(None, 'px')
- b_factor: float32 [64, 2048], P(None, 'py')
- c_factor: float32 [64, 32], P(None, 'fr')
The draws below stay inside these ranges and needn't reach their ends.
Inputs may be any that keep to these rules, and one draw needn't show every extreme that they name: `b_start`: entries are positive. `c_start`: entries are positive.
All inputs are finite; a program needn't handle non-finite values.
Results may differ from the reference program's by a relative error of at most 0.0003.
Values sent between devices are 32-bit elements; how exact they have to be, the bound alone decides.
A program may use at most 64 MiB of HBM per device.

```python
import math
import jax
import jax.numpy as jnp
from jax import lax

R = 64
PASSES = 4
I = 2048
J = 2048
K = 32


def rising_factor(key, rows, length):
    low = math.log(0.1)
    base = jnp.exp(jax.random.uniform(key, (rows, length), jnp.float32, low, 0.0))
    top = math.log(5.0)
    place = jnp.arange(length, dtype=jnp.float32) / max(length - 1, 1)
    return base * jnp.exp(top * place)[None, :]


def draw_b_start(key, part):
    return rising_factor(jax.random.fold_in(key, 11), R, J)


def draw_c_start(key, part):
    return rising_factor(jax.random.fold_in(key, 23), R, K)


def shard_levels(own_key, dims, cuts, smallest, high):
    level, own = 1.0, jax.random.fold_in(own_key, 6)
    for dim, parts in cuts:
        draws = jnp.exp(jax.random.uniform(jax.random.fold_in(own, dim), (parts,), jnp.float32, smallest / len(cuts), high / len(cuts)))
        level = level * jnp.repeat(draws, dims[dim] // parts).reshape([-1 if axis == dim else 1 for axis in range(len(dims))])
    return level


def setup_inputs(seed: int = 0) -> dict:
    key_list = jax.random.split(jax.random.key(seed), 5)
    return {
        "frames": jnp.clip(jnp.exp(math.log(1.0) - 3.9171631 * jax.random.uniform(key_list[0], (K, I, J), jnp.float32) ** shard_levels(key_list[0], (K, I, J), ((0, 8), (1, 4), (2, 8)), -0.2, 0.2)), 0.019897461, 1.0).astype(jnp.bfloat16),
        "a_start": jnp.clip(jnp.exp(math.log(1.0) - 2.3025851 * jax.random.uniform(key_list[1], (R, I), jnp.float32) ** shard_levels(key_list[1], (R, I), ((1, 4),), -0.2, 0.2)), 0.1, 1.0),
        "b_start": draw_b_start(jax.random.fold_in(key_list[4], 71), 0),
        "c_start": draw_c_start(jax.random.fold_in(key_list[4], 71), 0),
    }


def gram_matrix(factor):
    return jnp.dot(factor, factor.T, precision=lax.Precision.HIGHEST, preferred_element_type=jnp.float32)


def refresh(factor, mttkrp, hadamard):
    lower = jnp.dot(hadamard, factor, precision=lax.Precision.HIGHEST, preferred_element_type=jnp.float32)
    return factor * mttkrp / lower


def reference(frames, a_start, b_start, c_start):
    a_factor, b_factor, c_factor = a_start, b_start, c_start
    gram_b = gram_matrix(b_factor)
    gram_c = gram_matrix(c_factor)
    for pass_index in range(PASSES):
        b_half = b_factor.astype(jnp.bfloat16)

        def over_second(slab):
            return lax.dot_general(b_half, slab, (((1,), (1,)), ((), ())), preferred_element_type=jnp.float32)

        partial_a = lax.map(over_second, frames)
        mttkrp_a = jnp.einsum('kri,rk->ri', partial_a, c_factor, precision=lax.Precision.HIGHEST)
        a_factor = refresh(a_factor, mttkrp_a, gram_b * gram_c)
        gram_a = gram_matrix(a_factor)
        a_half = a_factor.astype(jnp.bfloat16)

        def over_first(slab):
            return jnp.dot(a_half, slab, preferred_element_type=jnp.float32)

        shared = lax.map(over_first, frames)
        mttkrp_b = jnp.einsum('krj,rk->rj', shared, c_factor, precision=lax.Precision.HIGHEST)
        b_factor = refresh(b_factor, mttkrp_b, gram_a * gram_c)
        gram_b = gram_matrix(b_factor)
        mttkrp_c = jnp.einsum('krj,rj->rk', shared, b_factor, precision=lax.Precision.HIGHEST)
        c_factor = refresh(c_factor, mttkrp_c, gram_a * gram_b)
        gram_c = gram_matrix(c_factor)
    return a_factor, b_factor, c_factor
```

```python
import functools

import jax
import jax.numpy as jnp
from jax import lax
from jax.experimental import pallas as pl
from jax.experimental.pallas import tpu as pltpu
from jax.sharding import PartitionSpec as P

PASSES = 4
HI = lax.Precision.HIGHEST
F32 = jnp.float32
BF16 = jnp.bfloat16


def nt(x, y):
    return lax.dot_general(x, y, (((1,), (1,)), ((), ())), precision=HI, preferred_element_type=F32)


class Group:
    def __init__(self, axis, size):
        self.axis, self.size, self.me = axis, size, lax.axis_index(axis)
        half = size // 2
        self.offsets = sorted(range(1, size), key=lambda d: -min(d, size - d))

    def peer(self, d):
        return lax.rem(self.me + d, self.size)

    def source(self, d):
        return lax.rem(self.me + self.size - d, self.size)

    def copy(self, src, dst, sems, d):
        return pltpu.make_async_remote_copy(
            src_ref=src,
            dst_ref=dst,
            send_sem=sems.at[0, d],
            recv_sem=sems.at[1, d],
            device_id={self.axis: self.peer(d)},
            device_id_type=pl.DeviceIdType.MESH,
        )

    def start(self, src_for, dst, sems):
        copies = [self.copy(src_for(self.peer(d)), dst(self.me), sems, d) for d in self.offsets]
        for c in copies:
            c.start()
        return copies

    def arrive(self, dst, sems):
        for d in reversed(self.offsets):
            slot = dst(self.source(d))
            self.copy(slot, slot, sems, d).wait_recv()


def kernel(
    sizes,
    frames,
    a_start,
    b_start,
    c_start,
    a_out,
    b_out,
    c_out,
    a_buf,
    b_buf,
    local_a,
    local_b,
    shared,
    ra,
    za,
    rb,
    yb,
    yc,
    zc,
    cg,
    ga,
    gb,
    h_ref,
    s_ra,
    s_za,
    s_ga,
    s_rb,
    s_yb,
    s_gb,
    s_yc,
    s_zc,
    s_cg,
    s_aa,
    s_ab,
):
    npx, npy, nfr = sizes
    ys, zs, fs = Group("px", npx), Group("py", npy), Group("fr", nfr)
    groups = (ys, zs, fs)
    rank, i_len = a_start.shape
    j_len = b_start.shape[1]
    kk = c_start.shape[1]
    rows = rank // nfr
    own = pl.ds(pl.multiple_of(fs.me * rows, rows), rows)

    def block(f):
        return pl.ds(pl.multiple_of(f * rows, rows), rows)

    barrier = pltpu.get_barrier_semaphore()
    for g in groups:
        for d in g.offsets:
            pl.semaphore_signal(
                barrier, inc=1, device_id={g.axis: g.peer(d)}, device_id_type=pl.DeviceIdType.MESH
            )

    eye = lax.broadcasted_iota(jnp.int32, (rank, rank), 0) == lax.broadcasted_iota(
        jnp.int32, (rank, rank), 1
    )
    live = (lax.broadcasted_iota(jnp.int32, (8, 128), 0) < kk) & (
        lax.broadcasted_iota(jnp.int32, (8, 128), 1) < rank
    )

    def tile_of(columns):
        turned = [jnp.sum(jnp.where(eye, c, 0.0), axis=0, keepdims=True) for c in columns]
        low = jnp.concatenate(turned + [jnp.zeros((8 - kk, rank), F32)], axis=0)
        return jnp.concatenate([low, jnp.zeros((8, 128 - rank), F32)], axis=1)

    def columns_of(tile):
        return [
            jnp.sum(jnp.where(eye, tile[k : k + 1, :rank], 0.0), axis=1, keepdims=True)
            for k in range(kk)
        ]

    def packed(gram):
        return jnp.concatenate([gram[: rank // 2], gram[rank // 2 :]], axis=1)

    def unpacked(pack):
        return jnp.concatenate([pack[:, :rank], pack[:, rank:]], axis=0)

    def total(ref, n):
        out = ref[0]
        for s in range(1, n):
            out = out + ref[s]
        return out

    def make_local_a(b, c_cols):
        b_half = b.astype(BF16)
        out = None
        for k in range(kk):
            part = lax.dot_general(
                b_half, frames[k], (((1,), (1,)), ((), ())), preferred_element_type=F32
            )
            out = c_cols[k] * part if out is None else out + c_cols[k] * part
        local_a[...] = out

    a_buf[0] = a_start[...]
    b_buf[0] = b_start[...]
    c_cols = [c_start[:, k : k + 1] for k in range(kk)]
    cg[fs.me] = tile_of(c_cols)
    gb[zs.me] = packed(nt(b_start[...], b_start[...]))

    pl.semaphore_wait(barrier, sum(g.size - 1 for g in groups))
    pending = []
    pending += zs.start(lambda p: gb.at[zs.me], lambda s: gb.at[s], s_gb)
    pending += fs.start(lambda p: cg.at[fs.me], lambda s: cg.at[s], s_cg)

    def flush(pending):
        for c in pending:
            c.wait_send()
        pending.clear()

    gram_b = None
    for step in range(PASSES):
        now, new = step % 2, (step + 1) % 2
        make_local_a(b_buf[now], c_cols)
        sent = fs.start(lambda p: local_a.at[block(p)], lambda s: ra.at[s], s_ra)
        fs.arrive(lambda s: cg.at[s], s_cg)
        if gram_b is None:
            zs.arrive(lambda s: gb.at[s], s_gb)
            gram_b = unpacked(total(gb, npy))
        every_c = cg[...].reshape(nfr * 8, 128)
        gram_c = lax.dot_general(
            every_c, every_c, (((0,), (0,)), ((), ())), precision=HI, preferred_element_type=F32
        )[:rank, :rank]
        h_ref[...] = gram_b * gram_c
        lower = jnp.dot(h_ref[own, :], a_buf[now], precision=HI, preferred_element_type=F32)
        scale = a_buf[now, own, :]
        flush(pending)
        ra[fs.me] = local_a[own, :]
        fs.arrive(lambda s: ra.at[s], s_ra)
        za[zs.me] = total(ra, nfr)
        pending += sent
        sent = zs.start(lambda p: za.at[zs.me], lambda s: za.at[s], s_za)
        flush(pending)
        zs.arrive(lambda s: za.at[s], s_za)
        a_buf[new, own, :] = scale * total(za, npy) / lower
        pending += sent
        sent = fs.start(
            lambda p: a_buf.at[new, own, :], lambda s: a_buf.at[new, block(s), :], s_aa
        )
        flush(pending)
        fs.arrive(lambda s: a_buf.at[new, block(s), :], s_aa)
        pending += sent

        a_half = a_buf[new].astype(BF16)
        out = None
        for k in range(kk):
            part = jnp.dot(a_half, frames[k], preferred_element_type=F32)
            shared[k] = part
            out = c_cols[k] * part if out is None else out + c_cols[k] * part
        local_b[...] = out
        sent = fs.start(lambda p: local_b.at[block(p)], lambda s: rb.at[s], s_rb)
        ga[ys.me] = packed(nt(a_buf[new], a_buf[new]))
        sent += ys.start(lambda p: ga.at[ys.me], lambda s: ga.at[s], s_ga)
        rb[fs.me] = local_b[own, :]
        flush(pending)
        fs.arrive(lambda s: rb.at[s], s_rb)
        yb[ys.me] = total(rb, nfr)
        pending += sent
        sent = ys.start(lambda p: yb.at[ys.me], lambda s: yb.at[s], s_yb)
        ys.arrive(lambda s: ga.at[s], s_ga)
        gram_a = unpacked(total(ga, npx))
        h_ref[...] = gram_a * gram_c
        lower = jnp.dot(h_ref[own, :], b_buf[now], precision=HI, preferred_element_type=F32)
        scale = b_buf[now, own, :]
        flush(pending)
        ys.arrive(lambda s: yb.at[s], s_yb)
        b_buf[new, own, :] = scale * total(yb, npx) / lower
        pending += sent
        sent = fs.start(
            lambda p: b_buf.at[new, own, :], lambda s: b_buf.at[new, block(s), :], s_ab
        )
        flush(pending)
        fs.arrive(lambda s: b_buf.at[new, block(s), :], s_ab)
        pending += sent

        b_new = b_buf[new]
        yc[ys.me] = tile_of(
            [jnp.sum(shared[k] * b_new, axis=1, keepdims=True) for k in range(kk)]
        )
        sent = ys.start(lambda p: yc.at[ys.me], lambda s: yc.at[s], s_yc)
        gb[zs.me] = packed(nt(b_new, b_new))
        sent += zs.start(lambda p: gb.at[zs.me], lambda s: gb.at[s], s_gb)
        flush(pending)
        ys.arrive(lambda s: yc.at[s], s_yc)
        zc[zs.me] = total(yc, npx)
        pending += sent
        sent = zs.start(lambda p: zc.at[zs.me], lambda s: zc.at[s], s_zc)
        zs.arrive(lambda s: gb.at[s], s_gb)
        gram_b = unpacked(total(gb, npy))
        c_tile = cg[fs.me]
        lower = jnp.dot(
            c_tile[:, :rank], gram_a * gram_b, precision=HI, preferred_element_type=F32
        )
        lower = jnp.concatenate([lower, jnp.ones((8, 128 - rank), F32)], axis=1)
        flush(pending)
        zs.arrive(lambda s: zc.at[s], s_zc)
        c_tile = jnp.where(live, c_tile * total(zc, npy) / jnp.where(live, lower, 1.0), 0.0)
        c_cols = columns_of(c_tile)
        pending += sent
        if step + 1 < PASSES:
            cg[fs.me] = c_tile
            pending += fs.start(lambda p: cg.at[fs.me], lambda s: cg.at[s], s_cg)
    flush(pending)
    a_out[...] = a_buf[PASSES % 2]
    b_out[...] = b_buf[PASSES % 2]
    c_out[...] = jnp.concatenate(c_cols, axis=1)


def body(sizes, frames, a_start, b_start, c_start):
    npx, npy, nfr = sizes
    rank, i_len = a_start.shape
    j_len = b_start.shape[1]
    kk = c_start.shape[1]
    rows = rank // nfr
    vmem = pl.BlockSpec(memory_space=pltpu.VMEM)

    def sems(n):
        return pltpu.SemaphoreType.DMA((2, n))

    return pl.pallas_call(
        functools.partial(kernel, sizes),
        name="cp",
        out_shape=[
            jax.ShapeDtypeStruct((rank, i_len), F32),
            jax.ShapeDtypeStruct((rank, j_len), F32),
            jax.ShapeDtypeStruct((rank, kk), F32),
        ],
        in_specs=[vmem] * 4,
        out_specs=[vmem] * 3,
        scratch_shapes=[
            pltpu.VMEM((2, rank, i_len), F32),
            pltpu.VMEM((2, rank, j_len), F32),
            pltpu.VMEM((rank, i_len), F32),
            pltpu.VMEM((rank, j_len), F32),
            pltpu.VMEM((kk, rank, j_len), F32),
            pltpu.VMEM((nfr, rows, i_len), F32),
            pltpu.VMEM((npy, rows, i_len), F32),
            pltpu.VMEM((nfr, rows, j_len), F32),
            pltpu.VMEM((npx, rows, j_len), F32),
            pltpu.VMEM((npx, 8, 128), F32),
            pltpu.VMEM((npy, 8, 128), F32),
            pltpu.VMEM((nfr, 8, 128), F32),
            pltpu.VMEM((npx, rank // 2, 2 * rank), F32),
            pltpu.VMEM((npy, rank // 2, 2 * rank), F32),
            pltpu.VMEM((rank, rank), F32),
            sems(nfr),
            sems(npy),
            sems(npx),
            sems(nfr),
            sems(npx),
            sems(npy),
            sems(npx),
            sems(npy),
            sems(nfr),
            sems(nfr),
            sems(nfr),
        ],
        compiler_params=pltpu.CompilerParams(collective_id=0, has_side_effects=True),
    )(frames, a_start, b_start, c_start)


def solution(mesh):
    sizes = (mesh.shape["px"], mesh.shape["py"], mesh.shape["fr"])
    return jax.shard_map(
        functools.partial(body, sizes),
        mesh=mesh,
        in_specs=(P("fr", "px", "py"), P(None, "px"), P(None, "py"), P(None, "fr")),
        out_specs=(P(None, "px"), P(None, "py"), P(None, "fr")),
        check_vma=False,
    )
```

```python
import functools

import jax
import jax.numpy as jnp
from jax import lax
from jax.experimental import pallas as pl
from jax.experimental.pallas import tpu as pltpu
from jax.sharding import PartitionSpec as P

PASSES = 4
CORES = 2
HI = lax.Precision.HIGHEST
F32 = jnp.float32
BF16 = jnp.bfloat16
MESH = pl.DeviceIdType.MESH


def nt(x, y):
    return lax.dot_general(x, y, (((1,), (1,)), ((), ())), precision=HI, preferred_element_type=F32)


def far_first(offsets, sizes):
    def hops(o):
        return sum(min(d, n - d) for d, n in zip(o, sizes))

    return sorted(offsets, key=lambda o: (-hops(o), o))


def remote(src, dst, send, recv, device):
    return pltpu.make_async_remote_copy(
        src_ref=src, dst_ref=dst, send_sem=send, recv_sem=recv, device_id=device, device_id_type=MESH
    )


def kernel(
    sizes,
    frames,
    a_start,
    b_start,
    c_start,
    a_out,
    b_out,
    c_out,
    a_buf,
    b_buf,
    part_a,
    local_a,
    local_b,
    shared,
    ra,
    za,
    rb,
    yb,
    yzc,
    cg,
    ga,
    gb,
    h_ref,
    gram_c_ref,
    gram_b_ref,
    low_a,
    low_b,
    s_ra,
    s_za,
    s_aa,
    s_ga,
    s_rb,
    s_yb,
    s_ab,
    s_gb,
    s_yzc,
    s_cg,
):
    npx, npy, nfr = sizes
    nx = nfr // CORES
    y, z, fr = lax.axis_index("px"), lax.axis_index("py"), lax.axis_index("fr")
    x, core = fr // CORES, lax.rem(fr, CORES)
    lead, helper = core == 1, core == 0
    rank = a_start.shape[0]
    kk = c_start.shape[0]
    rows = rank // nx
    own = pl.ds(pl.multiple_of(x * rows, rows), rows)
    yz = y * npy + z

    def block(i):
        return pl.ds(pl.multiple_of(i * rows, rows), rows)

    def to_x(d):
        return lax.rem(x + d, nx)

    def from_x(d):
        return lax.rem(x + nx - d, nx)

    x_away = [d for d, in far_first([(d,) for d in range(1, nx)], (nx,))]
    y_away = [d for d, in far_first([(d,) for d in range(1, npx)], (npx,))]
    z_away = [d for d, in far_first([(d,) for d in range(1, npy)], (npy,))]
    yz_away = far_first(
        [(i, j) for i in range(npx) for j in range(npy) if i or j], (npx, npy)
    )

    class Transfers:
        def __init__(self, pairs):
            self.pairs = pairs

        def each(self, act):
            for when, c in self.pairs:
                if when is None:
                    act(c)
                else:
                    pl.when(when)(functools.partial(act, c))

        def start(self):
            self.each(lambda c: c.start())
            return self

        def sent(self):
            self.each(lambda c: c.wait_send())

        def arrived(self):
            self.each(lambda c: c.wait_recv())

    def to_owner(src, dst, sems):
        out = []
        for d in x_away + [0]:
            c = remote(
                src.at[block(to_x(d))],
                dst.at[fr],
                sems.at[0, d],
                sems.at[1, CORES * d + core],
                {"fr": CORES * to_x(d) + 1},
            )
            out.append((None if d else helper, c))
        return Transfers(out).start()

    def at_owner(dst, sems):
        out = []
        for d in [0] + x_away[::-1]:
            for s in (1, 0) if d else (0,):
                slot = dst.at[CORES * from_x(d) + s]
                out.append((None, remote(slot, slot, sems.at[0, 0], sems.at[1, CORES * d + s], {"fr": fr})))
        Transfers(out).arrived()

    def from_owner(buf, sems):
        out = []
        for d in x_away + [0]:
            for s in (0, 1) if d else (0,):
                out.append(
                    (
                        None,
                        remote(
                            buf.at[own],
                            buf.at[own],
                            sems.at[0, CORES * d + s],
                            sems.at[1, d],
                            {"fr": CORES * to_x(d) + s},
                        ),
                    )
                )
        return Transfers(out)

    def at_all(buf, sems):
        out = []
        for d in [0] + x_away[::-1]:
            slot = buf.at[block(from_x(d))]
            out.append((None if d else helper, remote(slot, slot, sems.at[0, 0], sems.at[1, d], {"fr": fr})))
        Transfers(out).arrived()

    def along(axis, me, n, away, dst, sems):
        def copy(d, slot):
            return remote(dst.at[slot], dst.at[slot], sems.at[0, d], sems.at[1, d], {axis: lax.rem(me + d, n)})

        out = Transfers([(None, copy(d, me)) for d in away])
        back = Transfers([(None, copy(d, lax.rem(me + n - d, n))) for d in away[::-1]])
        return out, back

    y_line = functools.partial(along, "px", y, npx, y_away)
    z_line = functools.partial(along, "py", z, npy, z_away)

    def plane(dst, sems):
        def copy(o, slot):
            k = o[0] * npy + o[1]
            there = {"px": lax.rem(y + o[0], npx), "py": lax.rem(z + o[1], npy)}
            return remote(dst.at[slot], dst.at[slot], sems.at[0, k], sems.at[1, k], there)

        def source(o):
            return lax.rem(y + npx - o[0], npx) * npy + lax.rem(z + npy - o[1], npy)

        out = Transfers([(None, copy(o, yz)) for o in yz_away])
        back = Transfers([(None, copy(o, source(o))) for o in yz_away[::-1]])
        return out, back

    barrier = pltpu.get_barrier_semaphore()
    for d in range(1, nfr):
        pl.semaphore_signal(barrier, inc=1, device_id={"fr": lax.rem(fr + d, nfr)}, device_id_type=MESH)
    for i, j in yz_away:
        there = {"px": lax.rem(y + i, npx), "py": lax.rem(z + j, npy)}
        pl.semaphore_signal(barrier, inc=1, device_id=there, device_id_type=MESH)

    eye = lax.broadcasted_iota(jnp.int32, (rank, rank), 0) == lax.broadcasted_iota(
        jnp.int32, (rank, rank), 1
    )

    def turned(column):
        return jnp.sum(jnp.where(eye, column, 0.0), axis=0, keepdims=True)

    def columns_of(c):
        return [
            jnp.sum(jnp.where(eye, c[k : k + 1, :], 0.0), axis=1, keepdims=True) for k in range(kk)
        ]

    def tile_of(c):
        low = jnp.concatenate([c, jnp.zeros((8 - kk, rank), F32)], axis=0)
        return jnp.concatenate([low, jnp.zeros((8, 128 - rank), F32)], axis=1)

    def packed(gram):
        return jnp.concatenate([gram[: rank // 2], gram[rank // 2 :]], axis=1)

    def unpacked(pack):
        return jnp.concatenate([pack[:, :rank], pack[:, rank:]], axis=0)

    def total(ref, n):
        out = ref[0]
        for s in range(1, n):
            out = out + ref[s]
        return out

    def multiply_a(b):
        b_half = b.astype(BF16)
        for k in range(kk):
            part_a[k] = lax.dot_general(
                b_half, frames[k], (((1,), (1,)), ((), ())), preferred_element_type=F32
            )

    a_buf[0] = a_start[...]
    b_buf[0] = b_start[...]
    c = c_start[...]
    c_cols = columns_of(c)
    cg[fr] = tile_of(c)

    to_lead, at_lead = [], []
    for d in x_away + [0]:
        to_lead.append(
            (
                None if d else helper,
                remote(
                    cg.at[fr], cg.at[fr], s_cg.at[0, d], s_cg.at[1, CORES * d + core], {"fr": CORES * to_x(d) + 1}
                ),
            )
        )
    c_send = Transfers(to_lead)
    gb_send, gb_back = z_line(gb, s_gb)
    za_send, za_back = z_line(za, s_za)
    ga_send, ga_back = y_line(ga, s_ga)
    yb_send, yb_back = y_line(yb, s_yb)
    yzc_send, yzc_back = plane(yzc, s_yzc)

    @pl.when(lead)
    def _():
        gb[z] = packed(nt(b_start[...], b_start[...]))

    pl.semaphore_wait(barrier, nfr - 1 + len(yz_away))
    @pl.when(lead)
    def _():
        gb_send.start()

    c_send.start()
    multiply_a(b_start[...])

    for step in range(PASSES):
        now, new = step % 2, (step + 1) % 2
        out = c_cols[0] * part_a[0]
        for k in range(1, kk):
            out = out + c_cols[k] * part_a[k]
        local_a[...] = out
        ra_send = to_owner(local_a, ra, s_ra)

        @pl.when(lead)
        def _():
            at_owner(cg, s_cg)
            if step == 0:
                gb_back.arrived()
                gb_send.sent()
                gram_b_ref[...] = unpacked(total(gb, npy))
            every_c = cg[...].reshape(nfr * 8, 128)
            gram_c = lax.dot_general(
                every_c, every_c, (((0,), (0,)), ((), ())), precision=HI, preferred_element_type=F32
            )[:rank, :rank]
            gram_c_ref[...] = gram_c
            h_ref[...] = gram_b_ref[...] * gram_c
            low_a[...] = jnp.dot(h_ref[own, :], a_buf[now], precision=HI, preferred_element_type=F32)
            ra[fr] = local_a[own, :]
            at_owner(ra, s_ra)
            za[z] = total(ra, nfr)
            za_send.start()

        c_send.sent()
        ra_send.sent()

        @pl.when(lead)
        def _():
            za_back.arrived()
            a_buf[new, own, :] = a_buf[now, own, :] * total(za, npy) / low_a[...]
            from_owner(a_buf.at[new], s_aa).start()
            za_send.sent()

        at_all(a_buf.at[new], s_aa)

        a_half = a_buf[new].astype(BF16)
        out = None
        for k in range(kk):
            part = jnp.dot(a_half, frames[k], preferred_element_type=F32)
            shared[k] = part
            out = c_cols[k] * part if out is None else out + c_cols[k] * part
        local_b[...] = out
        rb_send = to_owner(local_b, rb, s_rb)
        ga[y] = packed(nt(a_buf[new], a_buf[new]))
        ga_send.start()

        @pl.when(lead)
        def _():
            rb[fr] = local_b[own, :]
            at_owner(rb, s_rb)
            yb[y] = total(rb, nfr)
            yb_send.start()

        ga_back.arrived()
        gram_a = unpacked(total(ga, npx))

        @pl.when(lead)
        def _():
            h_ref[...] = gram_a * gram_c_ref[...]
            low_b[...] = jnp.dot(h_ref[own, :], b_buf[now], precision=HI, preferred_element_type=F32)
            yb_back.arrived()
            b_buf[new, own, :] = b_buf[now, own, :] * total(yb, npx) / low_b[...]
            from_owner(b_buf.at[new], s_ab).start()
            yb_send.sent()
            from_owner(a_buf.at[new], s_aa).sent()

        rb_send.sent()
        ga_send.sent()
        at_all(b_buf.at[new], s_ab)

        b_new = b_buf[new]
        rows_c = [turned(jnp.sum(shared[k] * b_new, axis=1, keepdims=True)) for k in range(kk)]
        yzc[yz] = jnp.concatenate(
            [jnp.concatenate(rows_c[k : k + 2], axis=1) for k in range(0, kk, 2)], axis=0
        )
        yzc_send.start()
        gb[z] = packed(nt(b_new, b_new))
        gb_send.start()
        if step + 1 < PASSES:
            multiply_a(b_new)

        @pl.when(lead)
        def _():
            from_owner(b_buf.at[new], s_ab).sent()

        gb_back.arrived()
        gram_b = unpacked(total(gb, npy))
        gram_b_ref[...] = gram_b
        lower = jnp.dot(c, gram_a * gram_b, precision=HI, preferred_element_type=F32)
        yzc_back.arrived()
        pairs = total(yzc, npx * npy)
        m = jnp.concatenate(
            [pairs[k // 2 : k // 2 + 1, k % 2 * rank : (k % 2 + 1) * rank] for k in range(kk)], axis=0
        )
        c = c * m / lower
        yzc_send.sent()
        gb_send.sent()
        if step + 1 < PASSES:
            cg[fr] = tile_of(c)
            c_send.start()
            c_cols = columns_of(c)
    a_out[...] = a_buf[PASSES % 2]
    b_out[...] = b_buf[PASSES % 2]
    c_out[...] = c


def body(sizes, frames, a_start, b_start, c_start):
    npx, npy, nfr = sizes
    nx = nfr // CORES
    rank, i_len = a_start.shape
    j_len = b_start.shape[1]
    kk = c_start.shape[1]
    rows = rank // nx
    vmem = pl.BlockSpec(memory_space=pltpu.VMEM)

    def sems(n):
        return pltpu.SemaphoreType.DMA((2, n))

    a, b, c = pl.pallas_call(
        functools.partial(kernel, sizes),
        name="cp",
        out_shape=[
            jax.ShapeDtypeStruct((rank, i_len), F32),
            jax.ShapeDtypeStruct((rank, j_len), F32),
            jax.ShapeDtypeStruct((kk, rank), F32),
        ],
        in_specs=[vmem] * 4,
        out_specs=[vmem] * 3,
        scratch_shapes=[
            pltpu.VMEM((2, rank, i_len), F32),
            pltpu.VMEM((2, rank, j_len), F32),
            pltpu.VMEM((kk, rank, i_len), F32),
            pltpu.VMEM((rank, i_len), F32),
            pltpu.VMEM((rank, j_len), F32),
            pltpu.VMEM((kk, rank, j_len), F32),
            pltpu.VMEM((nfr, rows, i_len), F32),
            pltpu.VMEM((npy, rows, i_len), F32),
            pltpu.VMEM((nfr, rows, j_len), F32),
            pltpu.VMEM((npx, rows, j_len), F32),
            pltpu.VMEM((npx * npy, kk // 2, 2 * rank), F32),
            pltpu.VMEM((nfr, 8, 128), F32),
            pltpu.VMEM((npx, rank // 2, 2 * rank), F32),
            pltpu.VMEM((npy, rank // 2, 2 * rank), F32),
            pltpu.VMEM((rank, rank), F32),
            pltpu.VMEM((rank, rank), F32),
            pltpu.VMEM((rank, rank), F32),
            pltpu.VMEM((rows, i_len), F32),
            pltpu.VMEM((rows, j_len), F32),
            sems(nfr),
            sems(npy),
            sems(nfr),
            sems(npx),
            sems(nfr),
            sems(npx),
            sems(nfr),
            sems(npy),
            sems(npx * npy),
            sems(nfr),
        ],
        compiler_params=pltpu.CompilerParams(collective_id=0, has_side_effects=True),
    )(frames, a_start, b_start, c_start.T)
    return a, b, c.T


def solution(mesh):
    sizes = (mesh.shape["px"], mesh.shape["py"], mesh.shape["fr"])
    return jax.shard_map(
        functools.partial(body, sizes),
        mesh=mesh,
        in_specs=(P("fr", "px", "py"), P(None, "px"), P(None, "py"), P(None, "fr")),
        out_specs=(P(None, "px"), P(None, "py"), P(None, "fr")),
        check_vma=False,
    )
```
